128 devices in a mesh: rep: 2 (over core), dp: 64 (over x, y, z).
Axes of the slice: x: 4, y: 4, z: 4, core: 2. Of those that a mesh axis runs over, the one named last changes fastest.
Arguments:
- x: bfloat16 [128, 2048, 1280], P(('rep', 'dp')), parts along dimension 0
- dy: bfloat16 [128, 2048, 1280], P(('rep', 'dp')), parts along dimension 0
- wq: bfloat16 [1, 1280, 3072], P(None, 'dp')
- wk: bfloat16 [1, 1280, 256], P(None, 'dp')
- wv: bfloat16 [1, 1280, 256], P(None, 'dp')
- wo: bfloat16 [1, 3072, 1280], P(None, 'dp')
- w_gate: bfloat16 [1, 1280, 3072], P(None, 'dp')
- w_up: bfloat16 [1, 1280, 3072], P(None, 'dp')
- w_down: bfloat16 [1, 3072, 1280], P(None, 'dp')
- m_wq: float32 [1, 1280, 3072], P(None, 'dp')
- m_wk: float32 [1, 1280, 256], P(None, 'dp')
- m_wv: float32 [1, 1280, 256], P(None, 'dp')
- m_wo: float32 [1, 3072, 1280], P(None, 'dp')
- m_w_gate: float32 [1, 1280, 3072], P(None, 'dp')
- m_w_up: float32 [1, 1280, 3072], P(None, 'dp')
- m_w_down: float32 [1, 3072, 1280], P(None, 'dp')
- v_wq: float32 [1, 1280, 3072], P(None, 'dp')
- v_wk: float32 [1, 1280, 256], P(None, 'dp')
- v_wv: float32 [1, 1280, 256], P(None, 'dp')
- v_wo: float32 [1, 3072, 1280], P(None, 'dp')
- v_w_gate: float32 [1, 1280, 3072], P(None, 'dp')
- v_w_up: float32 [1, 1280, 3072], P(None, 'dp')
- v_w_down: float32 [1, 3072, 1280], P(None, 'dp')
Outputs:
- output 1: bfloat16 [2, 1280, 3072], P('rep', 'dp'), parts along dimension 0
- output 2: bfloat16 [2, 1280, 256], P('rep', 'dp'), parts along dimension 0
- output 3: bfloat16 [2, 1280, 256], P('rep', 'dp'), parts along dimension 0
- output 4: bfloat16 [2, 3072, 1280], P('rep', 'dp'), parts along dimension 0
- output 5: bfloat16 [2, 1280, 3072], P('rep', 'dp'), parts along dimension 0
- output 6: bfloat16 [2, 1280, 3072], P('rep', 'dp'), parts along dimension 0
- output 7: bfloat16 [2, 3072, 1280], P('rep', 'dp'), parts along dimension 0
- output 8: float32 [2, 1280, 3072], P('rep', 'dp'), parts along dimension 0
- output 9: float32 [2, 1280, 256], P('rep', 'dp'), parts along dimension 0
- output 10: float32 [2, 1280, 256], P('rep', 'dp'), parts along dimension 0
- output 11: float32 [2, 3072, 1280], P('rep', 'dp'), parts along dimension 0
- output 12: float32 [2, 1280, 3072], P('rep', 'dp'), parts along dimension 0
- output 13: float32 [2, 1280, 3072], P('rep', 'dp'), parts along dimension 0
- output 14: float32 [2, 3072, 1280], P('rep', 'dp'), parts along dimension 0
- output 15: float32 [2, 1280, 3072], P('rep', 'dp'), parts along dimension 0
- output 16: float32 [2, 1280, 256], P('rep', 'dp'), parts along dimension 0
- output 17: float32 [2, 1280, 256], P('rep', 'dp'), parts along dimension 0
- output 18: float32 [2, 3072, 1280], P('rep', 'dp'), parts along dimension 0
- output 19: float32 [2, 1280, 3072], P('rep', 'dp'), parts along dimension 0
- output 20: float32 [2, 1280, 3072], P('rep', 'dp'), parts along dimension 0
- output 21: float32 [2, 3072, 1280], P('rep', 'dp'), parts along dimension 0
There are 2 independent parts. The reference program is written for one: setup_inputs(seed, part) draws one part's arguments, and reference() takes and returns one part's arrays. A program takes and returns all parts, laid end to end along the dimension named above; an argument that names none is the same for every part.
All inputs are finite; a program needn't handle non-finite values.
Results may differ from the reference program's by a relative error of at most 0.0243.
Values are sent between devices in bfloat16 or wider.
A program may use at most 1.5 GiB of HBM per device.

```python
import jax
import jax.numpy as jnp
from jax import lax

SEQUENCES = 64
TOKENS = 2048
D = 1280
HEADS = 24
KV_HEADS = 2
HEAD = 128
FF = 3072
LAYERS = 1
THETA = 10000
NAMES = ("wq", "wk", "wv", "wo", "w_gate", "w_up", "w_down")
SHAPES = {
    "wq": (LAYERS, D, HEADS * HEAD),
    "wk": (LAYERS, D, KV_HEADS * HEAD),
    "wv": (LAYERS, D, KV_HEADS * HEAD),
    "wo": (LAYERS, HEADS * HEAD, D),
    "w_gate": (LAYERS, D, FF),
    "w_up": (LAYERS, D, FF),
    "w_down": (LAYERS, FF, D),
}


def bump(key, n, height):
    away = (jnp.arange(n, dtype=jnp.int32) - jax.random.randint(key, (), 0, n, jnp.int32)) % n
    return jnp.where(away < n // 8, height, 1.0)


def together(key, own, strength):
    shared = jax.random.normal(key, own.shape[1:], jnp.float32)
    return (own + strength * shared) * lax.rsqrt(1 + strength * strength)


def setup_inputs(seed: int = 0, part: int = 0) -> dict:
    kx, kdy, ka, kb, kz, kf, kh, kl, *keys = jax.random.split(jax.random.key(seed), 8 + 3 * len(NAMES))
    kx, kdy, ka, kb = (jax.random.fold_in(k, part) for k in (kx, kdy, ka, kb))
    kw, km, kv = (keys[i::3] for i in range(3))
    shape = (SEQUENCES, TOKENS, D)
    much_x, much_dy = jax.random.uniform(kz, (2,), jnp.float32, 0.0, 1.0)
    loud = 2.0 ** jax.random.uniform(jax.random.fold_in(kz, 1), (), jnp.float32, -1.0, 2.0)
    layers = 2.0 ** jax.random.uniform(kl, (LAYERS, 1, 1), jnp.float32, -1.0, 1.0)
    times = {"wq": 1.0, "wk": 1.0, "wv": 2.0, "wo": layers, "w_gate": 1.0, "w_up": bump(kh, FF, 4.0), "w_down": layers}
    x = together(ka, jax.random.normal(kx, shape, jnp.float32), much_x) * bump(kf, D, 4.0)
    dy = together(kb, jax.random.normal(kdy, shape, jnp.float32), much_dy)
    drawn = {"x": x.astype(jnp.bfloat16), "dy": (loud * dy * (SEQUENCES * TOKENS) ** -0.5).astype(jnp.bfloat16)}
    for key, name in zip(kw, NAMES, strict=True):
        drawn[name] = (jax.random.normal(key, SHAPES[name], jnp.float32) * SHAPES[name][1] ** -0.5 * times[name]).astype(jnp.bfloat16)
    for key, name in zip(km, NAMES, strict=True):
        drawn[f"m_{name}"] = 0.1 * jax.random.normal(key, SHAPES[name], jnp.float32)
    for key, name in zip(kv, NAMES, strict=True):
        drawn[f"v_{name}"] = loud * loud * jax.random.uniform(key, SHAPES[name], jnp.float32, 0.2, 0.6)
    return drawn


def matmul(a, w):
    return jnp.dot(a, w, preferred_element_type=jnp.float32).astype(jnp.bfloat16)


def normed(h):
    wide = h.astype(jnp.float32)
    scale = lax.rsqrt(jnp.mean(wide**2, -1, keepdims=True) + 1e-6)
    return (wide * scale).astype(jnp.bfloat16)


def turned(t, theta):
    half = t.shape[-1] // 2
    angle = jnp.arange(t.shape[0], dtype=jnp.float32)[:, None] * theta ** (-jnp.arange(half, dtype=jnp.float32) / half)
    cos, sin = jnp.cos(angle)[:, None], jnp.sin(angle)[:, None]
    a, b = t[..., :half].astype(jnp.float32), t[..., half:].astype(jnp.float32)
    return jnp.concatenate([a * cos - b * sin, b * cos + a * sin], -1).astype(jnp.bfloat16)


def seen_by(q, k, v):
    tokens, kv = q.shape[0], k.shape[1]
    q = q.reshape(tokens, kv, -1, q.shape[-1])
    scores = jnp.einsum("tgsd,ugd->gstu", q.astype(jnp.float32), k.astype(jnp.float32)) * q.shape[-1] ** -0.5
    place = jnp.arange(tokens)
    weights = jax.nn.softmax(jnp.where(place[:, None] >= place, scores, -jnp.inf), -1).astype(jnp.bfloat16)
    return jnp.einsum("gstu,ugd->tgsd", weights.astype(jnp.float32), v.astype(jnp.float32)).astype(jnp.bfloat16).reshape(tokens, -1)


def layer(h, w):
    a = normed(h)
    q, k = (turned(matmul(a, w[name]).reshape(h.shape[0], -1, HEAD), THETA) for name in ("wq", "wk"))
    h = h + matmul(seen_by(q, k, matmul(a, w["wv"]).reshape(h.shape[0], -1, HEAD)), w["wo"])
    b = normed(h)
    gate = jnp.dot(b, w["w_gate"], preferred_element_type=jnp.float32)
    up = jnp.dot(b, w["w_up"], preferred_element_type=jnp.float32)
    return h + matmul((jax.nn.silu(gate) * up).astype(jnp.bfloat16), w["w_down"])


def adamw(w, m, v, g):
    m = 0.9 * m + 0.1 * g
    v = 0.95 * v + 0.05 * g * g
    step = m * lax.rsqrt(v + 1e-8) + 0.1 * w
    return (w - 0.02 * step).astype(jnp.bfloat16), m, v


def stack(weights, h):
    return lax.scan(lambda h, w: (layer(h, w), None), h, weights)[0]


def reference(x, dy, wq, wk, wv, wo, w_gate, w_up, w_down, m_wq, m_wk, m_wv, m_wo, m_w_gate, m_w_up, m_w_down, v_wq, v_wk, v_wv, v_wo, v_w_gate, v_w_up, v_w_down):
    weights = dict(zip(NAMES, (wq, wk, wv, wo, w_gate, w_up, w_down), strict=True))

    def take(so_far, sequence):
        h, by_y = sequence
        _, back = jax.vjp(stack, weights, h)
        by_weights, by_h = back(by_y)
        return jax.tree.map(lambda total, term: total + term.astype(jnp.float32), so_far, by_weights), by_h

    none_yet = {name: jnp.zeros(w.shape, jnp.float32) for name, w in weights.items()}
    by_weights, by_x = lax.scan(take, none_yet, (x, dy))
    gradients = [by_weights[name].astype(jnp.bfloat16).astype(jnp.float32) for name in NAMES]
    first = (m_wq, m_wk, m_wv, m_wo, m_w_gate, m_w_up, m_w_down)
    second = (v_wq, v_wk, v_wv, v_wo, v_w_gate, v_w_up, v_w_down)
    new = [adamw(weights[name].astype(jnp.float32), m, v, g) for name, m, v, g in zip(NAMES, first, second, gradients, strict=True)]
    return tuple(one[which] for which in range(3) for one in new)
```

```python
import jax
import jax.numpy as jnp
from jax import lax
from jax.experimental import pallas as pl
from jax.experimental.pallas import tpu as pltpu
from jax.sharding import PartitionSpec as P


MESH = pl.DeviceIdType.MESH
NEG = -1e30
HIDDEN = 2 * NEG
LOG2E = 1.4426950408889634
VMEM = 56 * 2**20
HEAD = 128
HALF = HEAD // 2
THETA = 10000
GROUP = 12
WIDE = 512
F32, BF16 = jnp.float32, jnp.bfloat16
SCALE = HEAD**-0.5


def _dot(a, b, ca, cb):
    return lax.dot_general(a, b, (((ca,), (cb,)), ((), ())), preferred_element_type=F32)


STEP = {"x": 16, "y": 4, "z": 1}


def _place(me, axis):
    return lax.rem(lax.div(me, STEP[axis]), 4)


def _peer(me, axis, ahead):
    here = _place(me, axis)
    there = lax.rem(here + ahead, 4)
    return there, me + (there - here) * STEP[axis]


def _greet(jobs):
    me, rep = lax.axis_index("dp"), lax.axis_index("rep")
    barrier = pltpu.get_barrier_semaphore()
    axes = sorted({job[1] for job in jobs})
    for axis in axes:
        for ahead in (1, 2, 3):
            pl.semaphore_signal(barrier, inc=1, device_id=(rep, _peer(me, axis, ahead)[1]), device_id_type=MESH)
    pl.semaphore_wait(barrier, 3 * len(axes))


def _copies(jobs, srcs, dsts, send, recv):
    me, rep = lax.axis_index("dp"), lax.axis_index("rep")
    copies = []
    for n, ((_, axis, (a, b)), src, dst) in enumerate(zip(jobs, srcs, dsts)):
        for j in (1, 0, 2):
            there, peer = _peer(me, axis, j + 1)
            copies.append(pltpu.make_async_remote_copy(
                src_ref=src.at[:, there, :, a:b], dst_ref=dst.at[j], send_sem=send.at[3 * n + j], recv_sem=recv.at[3 * n + j],
                device_id=(rep, peer), device_id_type=MESH))
    return copies


def _call(body, jobs, number, grid, args, in_specs, out_shape, out_specs, scratch, cost=None):
    n_in, n_out, n_jobs = len(args), len(out_shape), len(jobs)

    def kernel(*refs):
        ins, refs = refs[:n_in], refs[n_in:]
        srcs, refs = refs[:n_jobs], refs[n_jobs:]
        outs, refs = refs[:n_out], refs[n_out:]
        dsts, refs = refs[:n_jobs], refs[n_jobs:]
        rest, (send, recv) = refs[:-2], refs[-2:]

        def begin():
            _greet(jobs)
            for copy in _copies(jobs, srcs, dsts, send, recv):
                copy.start()

        def end():
            for copy in _copies(jobs, srcs, dsts, send, recv):
                copy.wait()

        if body is None:
            begin()
            end()
        else:
            pl.when(pl.program_id(0) == 0)(begin)
            body(*ins, *outs, *rest)
            pl.when(pl.program_id(0) == pl.num_programs(0) - 1)(end)

    anywhere = pl.BlockSpec(memory_space=pl.ANY)
    shapes = [jax.ShapeDtypeStruct((3, s.shape[0], s.shape[2], b - a), BF16) for s, _, (a, b) in jobs]
    got = pl.pallas_call(
        kernel,
        grid=grid,
        in_specs=[*in_specs, *[anywhere] * n_jobs],
        out_specs=[*out_specs, *[anywhere] * n_jobs],
        out_shape=[*out_shape, *shapes],
        scratch_shapes=[*scratch, pltpu.SemaphoreType.DMA((3 * n_jobs,)), pltpu.SemaphoreType.DMA((3 * n_jobs,))],
        compiler_params=pltpu.CompilerParams(
            collective_id=number, has_side_effects=True, vmem_limit_bytes=VMEM,
            dimension_semantics=("arbitrary",) * len(grid) if grid else None),
        cost_estimate=cost,
    )(*args, *[s for s, _, _ in jobs])
    return got[:n_out], got[n_out:]


class Part:
    def __init__(self, gradient, rows, order, columns=None):
        self.rows, self.left, self.order = rows, ["x", "y", "z"], list(order)
        self.columns = columns or (0, gradient.shape[1])
        self.now = gradient

    def job(self):
        at = self.left.index(self.order[0])
        many = 4 ** (len(self.left) - 1 - at) * self.rows
        self.now = self.now.reshape(4**at, 4, many, -1)
        return self.now, self.order[0], self.columns

    def take(self, got):
        axis = self.order.pop(0)
        a, b = self.columns
        own = lax.dynamic_index_in_dim(self.now, _place(lax.axis_index("dp"), axis), 1, keepdims=False)[..., a:b]
        total = own.astype(F32) + got[0].astype(F32) + got[1].astype(F32) + got[2].astype(F32)
        self.left.remove(axis)
        self.columns = (0, b - a)
        self.now = total.astype(BF16).reshape(-1, b - a)


def _roped(t, cos, sin):
    return t * cos + pltpu.roll(t, HALF, 1) * sin


def _forward(q_ref, k_ref, v_ref, cos_ref, sin_ref, o_ref, lse_ref, q_s, top_s, mix_s):
    bq = q_ref.shape[0]
    cols = GROUP * bq
    e = SCALE * LOG2E
    iq = pl.program_id(1)
    cos, sin = cos_ref[...], sin_ref[...]
    for n in range(GROUP):
        q_s[n * bq : (n + 1) * bq, :] = _roped(q_ref[:, n * HEAD : (n + 1) * HEAD].astype(F32), cos, sin).astype(BF16)
    top_s[...] = jnp.full(top_s.shape, NEG, F32)
    mix_s[...] = jnp.zeros(mix_s.shape, F32)
    strips = range(0, cols, WIDE)

    def block(start, bk, masked):
        here = pl.ds(pl.multiple_of(start, bk), bk)
        keys = k_ref[here, :]
        scores = [_dot(keys, q_s[at : at + WIDE, :], 1, 1) for at in strips]
        if masked:
            ok = lax.rem(lax.broadcasted_iota(jnp.int32, (bk, WIDE), 1), bq) >= lax.broadcasted_iota(jnp.int32, (bk, WIDE), 0)
        values = jnp.concatenate([v_ref[here, :].T, jnp.ones((8, bk), BF16)], axis=0)
        weights, keeps = [], []
        for at, s in zip(strips, scores):
            if masked:
                s = jnp.where(ok, s, HIDDEN)
            old = top_s[:, at : at + WIDE]
            top = jnp.maximum(old, s.max(axis=0, keepdims=True))
            top_s[:, at : at + WIDE] = top
            weights.append(jnp.exp2((s - top) * e).astype(BF16))
            keeps.append(jnp.exp2((old - top) * e))
        for at, p, keep in zip(strips, weights, keeps):
            mix_s[:, at : at + WIDE] = mix_s[:, at : at + WIDE] * keep + _dot(values, p, 1, 0)

    large = 2 * bq
    lax.fori_loop(0, lax.div(iq, 2), lambda j, _: block(j * large, large, False), None)
    pl.when(lax.rem(iq, 2) == 1)(lambda: block((iq - 1) * bq, bq, False))
    block(iq * bq, bq, True)

    total = mix_s[HEAD : HEAD + 1, :]
    out = (mix_s[:HEAD, :] * (1 / total)).T.astype(BF16)
    lse = top_s[...] * SCALE + jnp.log(total)
    for n in range(GROUP):
        o_ref[:, n * HEAD : (n + 1) * HEAD] = out[n * bq : (n + 1) * bq, :]
        lse_ref[0, n : n + 1, :] = lse[:, n * bq : (n + 1) * bq]


def attend(qkv, k, cos, sin, heads, kv):
    tokens, bq = qkv.shape[0], 256
    wide = GROUP * HEAD
    cols = GROUP * bq
    return pl.pallas_call(
        _forward,
        name="attend",
        grid=(kv, tokens // bq),
        in_specs=[
            pl.BlockSpec((bq, wide), lambda i, j: (j, i)),
            pl.BlockSpec((tokens, HEAD), lambda i, j: (0, i)),
            pl.BlockSpec((tokens, HEAD), lambda i, j: (0, heads + kv + i)),
            pl.BlockSpec((bq, HEAD), lambda i, j: (j, 0)),
            pl.BlockSpec((bq, HEAD), lambda i, j: (j, 0)),
        ],
        out_specs=[pl.BlockSpec((bq, wide), lambda i, j: (j, i)), pl.BlockSpec((1, GROUP, bq), lambda i, j: (i, 0, j))],
        out_shape=[jax.ShapeDtypeStruct((tokens, heads * HEAD), BF16), jax.ShapeDtypeStruct((kv, GROUP, tokens), F32)],
        scratch_shapes=[pltpu.VMEM((cols, HEAD), BF16), pltpu.VMEM((1, cols), F32), pltpu.VMEM((HEAD + 8, cols), F32)],
        compiler_params=pltpu.CompilerParams(dimension_semantics=("parallel", "arbitrary"), vmem_limit_bytes=VMEM),
        cost_estimate=pl.CostEstimate(flops=2 * tokens * tokens * heads * HEAD * 4, bytes_accessed=4 * tokens * heads * HEAD,
                                      transcendentals=heads * tokens * tokens),
    )(qkv, k, qkv, cos, sin)


def _backward(q_ref, k_ref, v_ref, do_ref, o_ref, lse_ref, cos_ref, sin_ref, dq_ref, dk_ref, dv_ref, q_s, do_s, row_s, dq_s, dk_s, dv_s):
    bq = q_ref.shape[0]
    cols = GROUP * bq
    e = SCALE * LOG2E
    iq = pl.program_id(0)

    @pl.when(iq == 0)
    def _():
        dk_s[...] = jnp.zeros(dk_s.shape, F32)
        dv_s[...] = jnp.zeros(dv_s.shape, F32)

    cos, sin = cos_ref[...], sin_ref[...]
    for n in range(GROUP):
        at, head = slice(n * bq, (n + 1) * bq), slice(n * HEAD, (n + 1) * HEAD)
        q_s[at, :] = _roped(q_ref[:, head].astype(F32), cos, sin).astype(BF16)
        by_out = do_ref[:, head]
        do_s[at, :] = by_out
        row_s[0:1, at] = lse_ref[0, n : n + 1, :] * LOG2E
        row_s[1:2, at] = (by_out.astype(F32) * o_ref[:, head].astype(F32)).T.sum(axis=0, keepdims=True)
    dq_s[...] = jnp.zeros(dq_s.shape, F32)
    strips = range(0, cols, WIDE)

    def block(start, bk, masked):
        here = pl.ds(pl.multiple_of(start, bk), bk)
        keys, values = k_ref[here, :], v_ref[here, :]
        scores = [_dot(keys, q_s[at : at + WIDE, :], 1, 1) for at in strips]
        dps = [_dot(values, do_s[at : at + WIDE, :], 1, 1) for at in strips]
        if masked:
            ok = lax.rem(lax.broadcasted_iota(jnp.int32, (bk, WIDE), 1), bq) >= lax.broadcasted_iota(jnp.int32, (bk, WIDE), 0)
        keys_t = keys.T
        for at, s, dp in zip(strips, scores, dps):
            p = jnp.exp2(s * e - row_s[0:1, at : at + WIDE])
            if masked:
                p = jnp.where(ok, p, 0.0)
            ds = (p * (dp - row_s[1:2, at : at + WIDE])).astype(BF16)
            dv_s[here, :] += _dot(p.astype(BF16), do_s[at : at + WIDE, :], 1, 0)
            dk_s[here, :] += _dot(ds, q_s[at : at + WIDE, :], 1, 0)
            dq_s[:, at : at + WIDE] += _dot(keys_t, ds, 1, 0)

    large = 4 * bq
    whole, over = lax.div(iq, 4), lax.rem(iq, 4)
    lax.fori_loop(0, whole, lambda j, _: block(j * large, large, False), None)
    pl.when(over >= 2)(lambda: block(whole * large, 2 * bq, False))
    pl.when(lax.rem(over, 2) == 1)(lambda: block((iq - 1) * bq, bq, False))
    block(iq * bq, bq, True)

    for n in range(GROUP):
        t = (dq_s[:, n * bq : (n + 1) * bq] * SCALE).T.astype(BF16).astype(F32)
        dq_ref[:, n * HEAD : (n + 1) * HEAD] = (t * cos + pltpu.roll(t * sin, HALF, 1)).astype(BF16)

    @pl.when(iq == pl.num_programs(0) - 1)
    def _():
        dk_ref[...] = (dk_s[...] * SCALE).astype(BF16)
        dv_ref[...] = dv_s[...].astype(BF16)


def attend_bwd(which, qkv, k, by_out, out, lse, cos, sin, heads, kv, jobs):
    tokens, bq = qkv.shape[0], 128
    wide, cols = GROUP * HEAD, GROUP * bq
    queries, turn = pl.BlockSpec((bq, wide), lambda j: (j, which)), pl.BlockSpec((bq, HEAD), lambda j: (j, 0))
    whole = pl.BlockSpec((tokens, HEAD), lambda j: (0, 0))
    return _call(
        _backward, jobs, which, (tokens // bq,),
        [qkv, k, qkv, by_out, out, lse, cos, sin],
        [queries, pl.BlockSpec((tokens, HEAD), lambda j: (0, which)), pl.BlockSpec((tokens, HEAD), lambda j: (0, heads + kv + which)),
         queries, queries, pl.BlockSpec((1, GROUP, bq), lambda j: (which, 0, j)), turn, turn],
        [jax.ShapeDtypeStruct((tokens, wide), BF16), jax.ShapeDtypeStruct((tokens, HEAD), BF16), jax.ShapeDtypeStruct((tokens, HEAD), BF16)],
        [pl.BlockSpec((bq, wide), lambda j: (j, 0)), whole, whole],
        [pltpu.VMEM((cols, HEAD), BF16), pltpu.VMEM((cols, HEAD), BF16), pltpu.VMEM((2, cols), F32), pltpu.VMEM((HEAD, cols), F32),
         pltpu.VMEM((tokens, HEAD), F32), pltpu.VMEM((tokens, HEAD), F32)],
        pl.CostEstimate(flops=2 * tokens * tokens * GROUP * HEAD * 5, bytes_accessed=8 * tokens * wide, transcendentals=GROUP * tokens * tokens),
    )


def matmul(a, w):
    return jnp.dot(a, w, preferred_element_type=F32).astype(BF16)


def normed(h):
    wide = h.astype(F32)
    scale = lax.rsqrt(jnp.mean(wide**2, -1, keepdims=True) + 1e-6)
    return (wide * scale).astype(BF16)


def turns(tokens):
    angle = jnp.arange(tokens, dtype=F32)[:, None] * THETA ** (-jnp.arange(HALF, dtype=F32) / HALF)
    cos, sin = jnp.cos(angle), jnp.sin(angle)
    return jnp.concatenate([cos, cos], 1), jnp.concatenate([-sin, sin], 1)


def swapped(t):
    return jnp.concatenate([t[:, HALF:], t[:, :HALF]], 1)


def adamw(w, m, v, g):
    m = 0.9 * m + 0.1 * g
    v = 0.95 * v + 0.05 * g * g
    step = m * lax.rsqrt(v + 1e-8) + 0.1 * w
    return (w - 0.02 * step).astype(BF16), m, v


def exchange(parts, number):
    jobs = [part.job() for part in parts]
    _, got = _call(None, jobs, number, (), [], [], [], [], [])
    for part, one in zip(parts, got):
        part.take(one)


def solution(mesh):
    def gathered(w):
        half = w.shape[0] // 2
        mine = lax.dynamic_slice_in_dim(w, lax.axis_index("rep") * half, half, 0)
        return lax.all_gather(mine, ("dp", "rep"), axis=0, tiled=True)

    def step(x, dy, *arrays):
        weights, m, v = (arrays[i : i + 7] for i in (0, 7, 14))
        wq, wk, wv, wo, w_gate, w_up, w_down = (w[0] for w in weights)
        x, dy = x[0], dy[0]
        tokens, wide, narrow, ff = x.shape[0], wq.shape[1], wk.shape[1], w_gate.shape[1]
        heads, kv = wide // HEAD, narrow // HEAD

        w_qkv = gathered(jnp.concatenate([wq, wk, wv], 1))
        wo_all = gathered(wo)
        w_in = gathered(jnp.concatenate([w_gate, w_up], 1))
        down_all = gathered(w_down)

        cos, sin = turns(tokens)
        a = normed(x)
        qkv = matmul(a, w_qkv)

        def roped(t):
            t = t.astype(F32)
            return (t * cos + swapped(t) * sin).astype(BF16)

        k = jnp.concatenate([roped(qkv[:, wide + n * HEAD : wide + (n + 1) * HEAD]) for n in range(kv)], 1)
        out, lse = attend(qkv, k, cos, sin, heads, kv)

        def later(out, wo, w_gate, w_up, w_down):
            h = x + matmul(out, wo)
            b = normed(h)
            gate = jnp.dot(b, w_gate, preferred_element_type=F32)
            up = jnp.dot(b, w_up, preferred_element_type=F32)
            return h + matmul((jax.nn.silu(gate) * up).astype(BF16), w_down)

        _, back = jax.vjp(later, out, wo_all, w_in[:, :ff], w_in[:, ff:], down_all)
        by_out, by_wo, by_gate, by_up, by_down = back(dy)

        few, many = wq.shape[0], wo.shape[0]
        mlp = [Part(by_gate, few, "xyz"), Part(by_up, few, "yxz"), Part(by_down, many, "zxy")]

        def unroped(t):
            t = t.astype(F32)
            return (t * cos + swapped(t * sin)).astype(BF16)

        def bwd(which, parts):
            (dq, dk, dv), got = attend_bwd(which, qkv, k, by_out, out, lse, cos, sin, heads, kv, [part.job() for part in parts])
            for part, one in zip(parts, got):
                part.take(one)
            by_q = matmul(a.T, dq)
            by_kv = matmul(a.T, jnp.concatenate([unroped(dk), dv], 1))
            cut = dq.shape[1] // 2
            return [Part(by_q, few, "xyz", (0, cut)), Part(by_q, few, "yxz", (cut, 2 * cut)), Part(by_kv, few, "xyz", (0, HEAD)),
                    Part(by_kv, few, "yxz", (HEAD, 2 * HEAD))]

        first = bwd(0, mlp)
        d = wo.shape[1]
        third = d // 3 // HEAD * HEAD
        wo_parts = [Part(by_wo, many, "xyz", (0, third)), Part(by_wo, many, "yzx", (third, 2 * third)), Part(by_wo, many, "zxy", (2 * third, d))]
        second = bwd(1, wo_parts + first + mlp)
        exchange(second + wo_parts + first + mlp, 2)
        exchange(second + wo_parts + first, 3)
        exchange(second, 4)

        (q0, q1, k0, v0), (q2, q3, k1, v1) = first, second
        sums = [[q0, q1, q2, q3], [k0, k1], [v0, v1], wo_parts, *[[part] for part in mlp]]
        gradients = [jnp.concatenate([part.now for part in some], 1) if len(some) > 1 else some[0].now for some in sums]
        new = [adamw(w.astype(F32), m, v, g.astype(F32)[None]) for w, m, v, g in zip(weights, m, v, gradients, strict=True)]
        return tuple(one[which] for which in range(3) for one in new)

    states, cut = P(("rep", "dp"), None, None), P(None, "dp", None)
    return jax.shard_map(
        step,
        mesh=mesh,
        in_specs=(states, states) + (cut,) * 21,
        out_specs=(P("rep", "dp", None),) * 21,
        check_vma=False,
    )
```

```python
import functools

import jax
import jax.numpy as jnp
from jax import lax
from jax.experimental import pallas as pl
from jax.experimental.pallas import tpu as pltpu
from jax.sharding import PartitionSpec as P


MESH = pl.DeviceIdType.MESH
NEG = -1e30
HIDDEN = 2 * NEG
LOG2E = 1.4426950408889634
VMEM = 56 * 2**20
HEAD = 128
HALF = HEAD // 2
THETA = 10000
GROUP = 12
WIDE = 512
F32, BF16 = jnp.float32, jnp.bfloat16
SCALE = HEAD**-0.5


def _dot(a, b, ca, cb):
    return lax.dot_general(a, b, (((ca,), (cb,)), ((), ())), preferred_element_type=F32)


STEP = {"x": 16, "y": 4, "z": 1}


def _place(me, axis):
    return lax.rem(lax.div(me, STEP[axis]), 4)


def _peer(me, axis, ahead):
    here = _place(me, axis)
    there = lax.rem(here + ahead, 4)
    return there, me + (there - here) * STEP[axis]


def _greet(jobs):
    me, rep = lax.axis_index("dp"), lax.axis_index("rep")
    barrier = pltpu.get_barrier_semaphore()
    axes = sorted({job[1] for job in jobs})
    for axis in axes:
        for ahead in (1, 2, 3):
            pl.semaphore_signal(barrier, inc=1, device_id=(rep, _peer(me, axis, ahead)[1]), device_id_type=MESH)
    pl.semaphore_wait(barrier, 3 * len(axes))


def _copies(jobs, srcs, dsts, send, recv):
    me, rep = lax.axis_index("dp"), lax.axis_index("rep")
    copies = []
    for n, ((_, axis, (a, b)), src, dst) in enumerate(zip(jobs, srcs, dsts)):
        for j in (1, 0, 2):
            there, peer = _peer(me, axis, j + 1)
            copies.append(pltpu.make_async_remote_copy(
                src_ref=src.at[:, there, :, a:b], dst_ref=dst.at[j], send_sem=send.at[3 * n + j], recv_sem=recv.at[3 * n + j],
                device_id=(rep, peer), device_id_type=MESH))
    return copies


def _call(body, jobs, number, grid, args, in_specs, out_shape, out_specs, scratch, cost=None):
    n_in, n_out, n_jobs = len(args), len(out_shape), len(jobs)

    def kernel(*refs):
        ins, refs = refs[:n_in], refs[n_in:]
        srcs, refs = refs[:n_jobs], refs[n_jobs:]
        outs, refs = refs[:n_out], refs[n_out:]
        dsts, refs = refs[:n_jobs], refs[n_jobs:]
        rest, (send, recv) = refs[:-2], refs[-2:]

        def begin():
            _greet(jobs)
            for copy in _copies(jobs, srcs, dsts, send, recv):
                copy.start()

        def end():
            for copy in _copies(jobs, srcs, dsts, send, recv):
                copy.wait()

        if body is None:
            begin()
            end()
        else:
            pl.when(pl.program_id(0) == 0)(begin)
            body(*ins, *outs, *rest)
            pl.when(pl.program_id(0) == pl.num_programs(0) - 1)(end)

    anywhere = pl.BlockSpec(memory_space=pl.ANY)
    shapes = [jax.ShapeDtypeStruct((3, s.shape[0], s.shape[2], b - a), BF16) for s, _, (a, b) in jobs]
    got = pl.pallas_call(
        kernel,
        grid=grid,
        in_specs=[*in_specs, *[anywhere] * n_jobs],
        out_specs=[*out_specs, *[anywhere] * n_jobs],
        out_shape=[*out_shape, *shapes],
        scratch_shapes=[*scratch, pltpu.SemaphoreType.DMA((3 * n_jobs,)), pltpu.SemaphoreType.DMA((3 * n_jobs,))],
        compiler_params=pltpu.CompilerParams(
            collective_id=number, has_side_effects=True, vmem_limit_bytes=VMEM,
            dimension_semantics=("arbitrary",) * len(grid) if grid else None),
        cost_estimate=cost,
    )(*args, *[s for s, _, _ in jobs])
    return got[:n_out], got[n_out:]


class Part:
    def __init__(self, gradient, rows, order, columns=None):
        self.rows, self.left, self.order = rows, ["x", "y", "z"], list(order)
        self.columns = columns or (0, gradient.shape[1])
        self.now = gradient

    def job(self):
        at = self.left.index(self.order[0])
        many = 4 ** (len(self.left) - 1 - at) * self.rows
        self.now = self.now.reshape(4**at, 4, many, -1)
        return self.now, self.order[0], self.columns

    def take(self, got):
        axis = self.order.pop(0)
        a, b = self.columns
        own = lax.dynamic_index_in_dim(self.now, _place(lax.axis_index("dp"), axis), 1, keepdims=False)[..., a:b]
        total = own.astype(F32) + got[0].astype(F32) + got[1].astype(F32) + got[2].astype(F32)
        self.left.remove(axis)
        self.columns = (0, b - a)
        self.now = total.astype(BF16).reshape(-1, b - a)


def _roped(t, cos, sin):
    return t * cos + pltpu.roll(t, HALF, 1) * sin


def _forward(q_ref, k_ref, v_ref, cos_ref, sin_ref, o_ref, lse_ref, q_s, top_s, mix_s):
    bq = q_ref.shape[0]
    cols = GROUP * bq
    e = SCALE * LOG2E
    iq = pl.program_id(1)
    cos, sin = cos_ref[...], sin_ref[...]
    for n in range(GROUP):
        q_s[n * bq : (n + 1) * bq, :] = _roped(q_ref[:, n * HEAD : (n + 1) * HEAD].astype(F32), cos, sin).astype(BF16)
    top_s[...] = jnp.full(top_s.shape, NEG, F32)
    mix_s[...] = jnp.zeros(mix_s.shape, F32)
    strips = range(0, cols, WIDE)

    def block(start, bk, masked):
        here = pl.ds(pl.multiple_of(start, bk), bk)
        keys = k_ref[here, :]
        scores = [_dot(keys, q_s[at : at + WIDE, :], 1, 1) for at in strips]
        if masked:
            ok = lax.rem(lax.broadcasted_iota(jnp.int32, (bk, WIDE), 1), bq) >= lax.broadcasted_iota(jnp.int32, (bk, WIDE), 0)
        values = jnp.concatenate([v_ref[here, :].T, jnp.ones((8, bk), BF16)], axis=0)
        weights, keeps = [], []
        for at, s in zip(strips, scores):
            if masked:
                s = jnp.where(ok, s, HIDDEN)
            old = top_s[:, at : at + WIDE]
            top = jnp.maximum(old, s.max(axis=0, keepdims=True))
            top_s[:, at : at + WIDE] = top
            weights.append(jnp.exp2((s - top) * e).astype(BF16))
            keeps.append(jnp.exp2((old - top) * e))
        for at, p, keep in zip(strips, weights, keeps):
            mix_s[:, at : at + WIDE] = mix_s[:, at : at + WIDE] * keep + _dot(values, p, 1, 0)

    large = 2 * bq
    lax.fori_loop(0, lax.div(iq, 2), lambda j, _: block(j * large, large, False), None)
    pl.when(lax.rem(iq, 2) == 1)(lambda: block((iq - 1) * bq, bq, False))
    block(iq * bq, bq, True)

    total = mix_s[HEAD : HEAD + 1, :]
    out = (mix_s[:HEAD, :] * (1 / total)).T.astype(BF16)
    lse = top_s[...] * SCALE + jnp.log(total)
    for n in range(GROUP):
        o_ref[:, n * HEAD : (n + 1) * HEAD] = out[n * bq : (n + 1) * bq, :]
        lse_ref[0, n : n + 1, :] = lse[:, n * bq : (n + 1) * bq]


def attend(qkv, k, cos, sin, heads, kv):
    tokens, bq = qkv.shape[0], 256
    wide = GROUP * HEAD
    cols = GROUP * bq
    return pl.pallas_call(
        _forward,
        name="attend",
        grid=(kv, tokens // bq),
        in_specs=[
            pl.BlockSpec((bq, wide), lambda i, j: (j, i)),
            pl.BlockSpec((tokens, HEAD), lambda i, j: (0, i)),
            pl.BlockSpec((tokens, HEAD), lambda i, j: (0, heads + kv + i)),
            pl.BlockSpec((bq, HEAD), lambda i, j: (j, 0)),
            pl.BlockSpec((bq, HEAD), lambda i, j: (j, 0)),
        ],
        out_specs=[pl.BlockSpec((bq, wide), lambda i, j: (j, i)), pl.BlockSpec((1, GROUP, bq), lambda i, j: (i, 0, j))],
        out_shape=[jax.ShapeDtypeStruct((tokens, heads * HEAD), BF16), jax.ShapeDtypeStruct((kv, GROUP, tokens), F32)],
        scratch_shapes=[pltpu.VMEM((cols, HEAD), BF16), pltpu.VMEM((1, cols), F32), pltpu.VMEM((HEAD + 8, cols), F32)],
        compiler_params=pltpu.CompilerParams(dimension_semantics=("parallel", "arbitrary"), vmem_limit_bytes=VMEM),
        cost_estimate=pl.CostEstimate(flops=2 * tokens * tokens * heads * HEAD * 4, bytes_accessed=4 * tokens * heads * HEAD,
                                      transcendentals=heads * tokens * tokens),
    )(qkv, k, qkv, cos, sin)


def _backward(q_ref, k_ref, v_ref, do_ref, o_ref, lse_ref, cos_ref, sin_ref, dq_ref, dk_ref, dv_ref, q_s, do_s, row_s, dq_s, dk_s, dv_s):
    bq = q_ref.shape[0]
    cols = GROUP * bq
    e = SCALE * LOG2E
    iq = pl.program_id(0)

    @pl.when(iq == 0)
    def _():
        dk_s[...] = jnp.zeros(dk_s.shape, F32)
        dv_s[...] = jnp.zeros(dv_s.shape, F32)

    cos, sin = cos_ref[...], sin_ref[...]
    for n in range(GROUP):
        at, head = slice(n * bq, (n + 1) * bq), slice(n * HEAD, (n + 1) * HEAD)
        q_s[at, :] = _roped(q_ref[:, head].astype(F32), cos, sin).astype(BF16)
        by_out = do_ref[:, head]
        do_s[at, :] = by_out
        row_s[0:1, at] = lse_ref[0, n : n + 1, :] * LOG2E
        row_s[1:2, at] = (by_out.astype(F32) * o_ref[:, head].astype(F32)).T.sum(axis=0, keepdims=True)
    dq_s[...] = jnp.zeros(dq_s.shape, F32)
    strips = range(0, cols, WIDE)

    def block(start, bk, masked):
        here = pl.ds(pl.multiple_of(start, bk), bk)
        keys, values = k_ref[here, :], v_ref[here, :]
        scores = [_dot(keys, q_s[at : at + WIDE, :], 1, 1) for at in strips]
        dps = [_dot(values, do_s[at : at + WIDE, :], 1, 1) for at in strips]
        if masked:
            ok = lax.rem(lax.broadcasted_iota(jnp.int32, (bk, WIDE), 1), bq) >= lax.broadcasted_iota(jnp.int32, (bk, WIDE), 0)
        keys_t = keys.T
        for at, s, dp in zip(strips, scores, dps):
            p = jnp.exp2(s * e - row_s[0:1, at : at + WIDE])
            if masked:
                p = jnp.where(ok, p, 0.0)
            ds = (p * (dp - row_s[1:2, at : at + WIDE])).astype(BF16)
            dv_s[here, :] += _dot(p.astype(BF16), do_s[at : at + WIDE, :], 1, 0)
            dk_s[here, :] += _dot(ds, q_s[at : at + WIDE, :], 1, 0)
            dq_s[:, at : at + WIDE] += _dot(keys_t, ds, 1, 0)

    large = 2 * bq
    lax.fori_loop(0, lax.div(iq, 2), lambda j, _: block(j * large, large, False), None)
    pl.when(lax.rem(iq, 2) == 1)(lambda: block((iq - 1) * bq, bq, False))
    block(iq * bq, bq, True)

    for n in range(GROUP):
        t = (dq_s[:, n * bq : (n + 1) * bq] * SCALE).T.astype(BF16).astype(F32)
        dq_ref[:, n * HEAD : (n + 1) * HEAD] = (t * cos + pltpu.roll(t * sin, HALF, 1)).astype(BF16)

    @pl.when(iq == pl.num_programs(0) - 1)
    def _():
        dk_ref[...] = (dk_s[...] * SCALE).astype(BF16)
        dv_ref[...] = dv_s[...].astype(BF16)


def attend_bwd(which, qkv, k, by_out, out, lse, cos, sin, heads, kv, jobs):
    tokens, bq = qkv.shape[0], 256
    wide, cols = GROUP * HEAD, GROUP * bq
    queries, turn = pl.BlockSpec((bq, wide), lambda j: (j, which)), pl.BlockSpec((bq, HEAD), lambda j: (j, 0))
    whole = pl.BlockSpec((tokens, HEAD), lambda j: (0, 0))
    return _call(
        _backward, jobs, which, (tokens // bq,),
        [qkv, k, qkv, by_out, out, lse, cos, sin],
        [queries, pl.BlockSpec((tokens, HEAD), lambda j: (0, which)), pl.BlockSpec((tokens, HEAD), lambda j: (0, heads + kv + which)),
         queries, queries, pl.BlockSpec((1, GROUP, bq), lambda j: (which, 0, j)), turn, turn],
        [jax.ShapeDtypeStruct((tokens, wide), BF16), jax.ShapeDtypeStruct((tokens, HEAD), BF16), jax.ShapeDtypeStruct((tokens, HEAD), BF16)],
        [pl.BlockSpec((bq, wide), lambda j: (j, 0)), whole, whole],
        [pltpu.VMEM((cols, HEAD), BF16), pltpu.VMEM((cols, HEAD), BF16), pltpu.VMEM((2, cols), F32), pltpu.VMEM((HEAD, cols), F32),
         pltpu.VMEM((tokens, HEAD), F32), pltpu.VMEM((tokens, HEAD), F32)],
        pl.CostEstimate(flops=2 * tokens * tokens * GROUP * HEAD * 5, bytes_accessed=8 * tokens * wide, transcendentals=GROUP * tokens * tokens),
    )


def _fetch(x_ref, shard, a_ref, got, send, recv, send2, recv2, local, *, cut):
    step = pl.program_id(0)
    me, rep = lax.axis_index("dp"), lax.axis_index("rep")
    here = {axis: _place(me, axis) for axis in "xyz"}
    width = shard.shape[1]
    third = width // 3 // HEAD * HEAD + HEAD
    pieces = [(0, third, "xyz"), (third, 2 * third, "yzx"), (2 * third, cut, "zxy"), (cut, width, "zxy")]

    def spot(piece, done, at):
        a, b, _ = piece
        start = rep * cut + a if b <= cut else 2 * cut + rep * (width - cut) + a - cut
        index = [slice(None) if axis in done else at.get(axis, here[axis]) for axis in "xyz"]
        return got.at[index[0], index[1], index[2], :, pl.ds(pl.multiple_of(start, HEAD), b - a)]

    def ring(phase):
        copies = []
        for c, piece in enumerate(pieces):
            order = piece[2]
            mine = spot(piece, order[:phase], {})
            src = shard.at[:, piece[0] : piece[1]] if phase == 0 else mine
            for j in range(3):
                n = 12 * phase + 3 * c + j
                copies.append(pltpu.make_async_remote_copy(
                    src_ref=src, dst_ref=mine, send_sem=send.at[n], recv_sem=recv.at[n],
                    device_id=(rep, _peer(me, order[phase], j + 1)[1]), device_id_type=MESH))
        return copies

    def across(c, j):
        order = pieces[c][2]
        part = spot(pieces[c], order[:2], {order[2]: lax.rem(here[order[2]] + 4 - j, 4)})
        return pltpu.make_async_remote_copy(
            src_ref=part, dst_ref=part, send_sem=send2.at[4 * c + j], recv_sem=recv2.at[4 * c + j],
            device_id=(1 - rep, me), device_id_type=MESH)

    owns = [pltpu.make_async_copy(shard.at[:, piece[0] : piece[1]], spot(piece, "", {}), local.at[c]) for c, piece in enumerate(pieces)]

    @pl.when(step == 0)
    def _():
        barrier = pltpu.get_barrier_semaphore()
        for axis in "xyz":
            for ahead in (1, 2, 3):
                pl.semaphore_signal(barrier, inc=1, device_id=(rep, _peer(me, axis, ahead)[1]), device_id_type=MESH)
        pl.semaphore_signal(barrier, inc=1, device_id=(1 - rep, me), device_id_type=MESH)
        pl.semaphore_wait(barrier, 10)
        for copy in ring(0):
            copy.start()
        for own in owns:
            own.start()

    a_ref[...] = normed(x_ref[...])

    @pl.when(step == 2)
    def _():
        for own in owns:
            own.wait()
        for copy in ring(0):
            copy.wait()
        for copy in ring(1):
            copy.start()

    @pl.when(step == 5)
    def _():
        for copy in ring(1):
            copy.wait()
        for copy in ring(2):
            copy.start()
        for c in range(4):
            across(c, 0).start()

    @pl.when(step == pl.num_programs(0) - 1)
    def _():
        last = ring(2)
        for j in (0, 2, 1):
            for c in range(4):
                last[3 * c + j].wait_recv()
                across(c, j + 1).start()
        for copy in last:
            copy.wait_send()
        for c in range(4):
            for j in range(4):
                across(c, j).wait()


def fetch(x, shard, cut, number):
    tokens, d = x.shape
    rows = pl.BlockSpec((tokens // 8, d), lambda i: (i, 0))
    anywhere = pl.BlockSpec(memory_space=pl.ANY)
    dma = pltpu.SemaphoreType.DMA
    return pl.pallas_call(
        functools.partial(_fetch, cut=cut),
        name="fetch",
        grid=(8,),
        in_specs=[rows, anywhere],
        out_specs=[rows, anywhere],
        out_shape=[jax.ShapeDtypeStruct((tokens, d), BF16), jax.ShapeDtypeStruct((4, 4, 4, shard.shape[0], 2 * shard.shape[1]), BF16)],
        scratch_shapes=[dma((36,)), dma((36,)), dma((16,)), dma((16,)), dma((4,))],
        compiler_params=pltpu.CompilerParams(
            collective_id=number, has_side_effects=True, vmem_limit_bytes=VMEM, dimension_semantics=("arbitrary",)),
        cost_estimate=pl.CostEstimate(flops=5 * 10**10, bytes_accessed=2 * 2 * tokens * d, transcendentals=0),
    )(x, shard)


def matmul(a, w):
    return jnp.dot(a, w, preferred_element_type=F32).astype(BF16)


def normed(h):
    wide = h.astype(F32)
    scale = lax.rsqrt(jnp.mean(wide**2, -1, keepdims=True) + 1e-6)
    return (wide * scale).astype(BF16)


def turns(tokens):
    angle = jnp.arange(tokens, dtype=F32)[:, None] * THETA ** (-jnp.arange(HALF, dtype=F32) / HALF)
    cos, sin = jnp.cos(angle), jnp.sin(angle)
    return jnp.concatenate([cos, cos], 1), jnp.concatenate([-sin, sin], 1)


def swapped(t):
    return jnp.concatenate([t[:, HALF:], t[:, :HALF]], 1)


def adamw(w, m, v, g):
    m = 0.9 * m + 0.1 * g
    v = 0.95 * v + 0.05 * g * g
    step = m * lax.rsqrt(v + 1e-8) + 0.1 * w
    return (w - 0.02 * step).astype(BF16), m, v


def exchange(parts, number):
    jobs = [part.job() for part in parts]
    _, got = _call(None, jobs, number, (), [], [], [], [], [])
    for part, one in zip(parts, got):
        part.take(one)


def solution(mesh):
    def gathered(w):
        half = w.shape[0] // 2
        mine = lax.dynamic_slice_in_dim(w, lax.axis_index("rep") * half, half, 0)
        return lax.all_gather(mine, ("dp", "rep"), axis=0, tiled=True)

    def step(x, dy, *arrays):
        weights, m, v = (arrays[i : i + 7] for i in (0, 7, 14))
        wq, wk, wv, wo, w_gate, w_up, w_down = (w[0] for w in weights)
        x, dy = x[0], dy[0]
        tokens, wide, narrow, ff = x.shape[0], wq.shape[1], wk.shape[1], w_gate.shape[1]
        heads, kv = wide // HEAD, narrow // HEAD

        cut = wide // 2
        first_group = lax.axis_index("rep") == 0
        shard = jnp.where(first_group, jnp.concatenate([wq[:, :cut], wk], 1), jnp.concatenate([wq[:, cut:], wv], 1))
        a, w_qkv = fetch(x, shard, cut, 5)
        wo_all = gathered(wo)
        w_in = gathered(jnp.concatenate([w_gate, w_up], 1))
        down_all = gathered(w_down)

        cos, sin = turns(tokens)
        w_qkv = w_qkv.reshape(-1, w_qkv.shape[-1])
        qkv = matmul(a, w_qkv)

        def roped(t):
            t = t.astype(F32)
            return (t * cos + swapped(t) * sin).astype(BF16)

        k = jnp.concatenate([roped(qkv[:, wide + n * HEAD : wide + (n + 1) * HEAD]) for n in range(kv)], 1)
        out, lse = attend(qkv, k, cos, sin, heads, kv)

        def later(out, wo, w_gate, w_up, w_down):
            h = x + matmul(out, wo)
            b = normed(h)
            gate = jnp.dot(b, w_gate, preferred_element_type=F32)
            up = jnp.dot(b, w_up, preferred_element_type=F32)
            return h + matmul((jax.nn.silu(gate) * up).astype(BF16), w_down)

        _, back = jax.vjp(later, out, wo_all, w_in[:, :ff], w_in[:, ff:], down_all)
        by_out, by_wo, by_gate, by_up, by_down = back(dy)

        few, many = wq.shape[0], wo.shape[0]
        mlp = [Part(by_gate, few, "xyz"), Part(by_up, few, "yxz"), Part(by_down, many, "zxy")]

        def unroped(t):
            t = t.astype(F32)
            return (t * cos + swapped(t * sin)).astype(BF16)

        def bwd(which, parts):
            (dq, dk, dv), got = attend_bwd(which, qkv, k, by_out, out, lse, cos, sin, heads, kv, [part.job() for part in parts])
            for part, one in zip(parts, got):
                part.take(one)
            by_q = matmul(a.T, dq)
            half = dq.shape[1] // 2
            return dk, dv, [Part(by_q, few, "xyz", (0, half)), Part(by_q, few, "yxz", (half, 2 * half))]

        dk0, dv0, first = bwd(0, mlp)
        d = wo.shape[1]
        third = d // 3 // HEAD * HEAD
        wo_parts = [Part(by_wo, many, "xyz", (0, third)), Part(by_wo, many, "yzx", (third, 2 * third)), Part(by_wo, many, "zxy", (2 * third, d))]
        dk1, dv1, second = bwd(1, wo_parts + first + mlp)
        by_kv = matmul(a.T, jnp.concatenate([unroped(dk0), unroped(dk1), dv0, dv1], 1))
        second += [Part(by_kv, few, "xyz", (0, narrow)), Part(by_kv, few, "yxz", (narrow, 2 * narrow))]
        exchange(second + wo_parts + first + mlp, 2)
        exchange(second + wo_parts + first, 3)
        exchange(second, 4)

        (q0, q1), (q2, q3, by_k, by_v) = first, second
        sums = [[q0, q1, q2, q3], [by_k], [by_v], wo_parts, *[[part] for part in mlp]]
        gradients = [jnp.concatenate([part.now for part in some], 1) if len(some) > 1 else some[0].now for some in sums]

        def flat(t):
            return t.reshape(-1, HEAD)

        new = [adamw(flat(w).astype(F32), flat(m), flat(v), flat(g).astype(F32)) for w, m, v, g in zip(weights, m, v, gradients, strict=True)]
        return tuple(one[which].reshape(w.shape) for which in range(3) for one, w in zip(new, weights))

    states, cut = P(("rep", "dp"), None, None), P(None, "dp", None)
    return jax.shard_map(
        step,
        mesh=mesh,
        in_specs=(states, states) + (cut,) * 21,
        out_specs=(P("rep", "dp", None),) * 21,
        check_vma=False,
    )
```
